32 devices in a mesh: rep: 1 (over z), dp: 4 (over y), ad: 8 (over x, core).
Axes of the slice: x: 4, y: 4, z: 1, core: 2. Of those that a mesh axis runs over, the one named last changes fastest.
The devices are a block of a 4x4x8 slice.
Arguments:
- x_rows: bfloat16 [16384, 1536], P(('rep', 'dp', 'ad'))
- adapter_id: int32 [16384], P(('rep', 'dp', 'ad'))
- w_gate: bfloat16 [1536, 8960], replicated
- w_up: bfloat16 [1536, 8960], replicated
- w_down: bfloat16 [8960, 1536], replicated
- a_gate: bfloat16 [32, 1536, 128], P('ad')
- b_gate: bfloat16 [32, 128, 8960], P('ad')
- a_up: bfloat16 [32, 1536, 128], P('ad')
- b_up: bfloat16 [32, 128, 8960], P('ad')
- a_down: bfloat16 [32, 8960, 128], P('ad')
- b_down: bfloat16 [32, 128, 1536], P('ad')
Outputs:
- output: bfloat16 [16384, 1536], P(('rep', 'dp', 'ad'))
All inputs are finite; a program needn't handle non-finite values.
Results may differ from the reference program's by a relative error of at most 0.00166.
Values are sent between devices in bfloat16 or wider.
A program may use at most 768 MiB of HBM per device.

```python
import jax
import jax.numpy as jnp
from jax import lax

D_MODEL = 1536
D_FF = 8960
RANK = 128
LORA_ALPHA = 32
TOKENS_DEV = 512
GROUP = 8
REPLICAS = 4
ADAPTERS = 32
ROW_BLOCK = 32
SOURCES = REPLICAS * GROUP
TOKENS = SOURCES * TOKENS_DEV
ADAPT_LOCAL = ADAPTERS // GROUP
CAPACITY = (TOKENS_DEV // GROUP) * min(4, max(1, GROUP // 2))


def draw_adapter_ids(key_ids):
    key_hot, key_off, key_perm, key_tok = jax.random.split(key_ids, 4)
    hot_base = jax.random.randint(key_hot, (), 0, GROUP)
    offset = jax.random.randint(key_off, (), 0, ADAPT_LOCAL)
    labels = jax.random.permutation(key_perm, ADAPT_LOCAL)
    source = jnp.arange(SOURCES)
    hot_owner = (hot_base + source // GROUP) % GROUP
    distance = (jnp.arange(GROUP)[None, :] - hot_owner[:, None]) % GROUP
    rest = TOKENS_DEV - CAPACITY
    cold_base = rest // (GROUP - 1)
    cold_extra = rest % (GROUP - 1)
    counts = jnp.where(distance == 0, CAPACITY, cold_base + (distance - 1 < cold_extra).astype(jnp.int32))
    owner_sorted = jax.vmap(lambda count_row: jnp.repeat(jnp.arange(GROUP), count_row, total_repeat_length=TOKENS_DEV))(counts)
    starts = jnp.cumsum(counts, axis=1) - counts
    within = jnp.arange(TOKENS_DEV)[None, :] - jnp.take_along_axis(starts, owner_sorted, axis=1)
    spread = within * SOURCES + source[:, None] + offset
    ids_sorted = owner_sorted * ADAPT_LOCAL + labels[spread % ADAPT_LOCAL]
    orders = jax.vmap(lambda sub_key: jax.random.permutation(sub_key, TOKENS_DEV))(jax.random.split(key_tok, SOURCES))
    return jnp.take_along_axis(ids_sorted, orders, axis=1).reshape(-1).astype(jnp.int32)


def setup_inputs(seed: int = 0, part: int = 0) -> dict:
    key_part = jax.random.fold_in(jax.random.key(seed), part)
    key_x, key_ids = jax.random.split(key_part)
    keys = jax.random.split(jax.random.key(seed + 1), 9)
    scale = LORA_ALPHA / RANK
    up_std = 0.4 / (scale * RANK ** 0.5)
    down_std = 0.5 / (scale * RANK ** 0.5)

    def normal(sub_key, shape, std_dev):
        return (jax.random.normal(sub_key, shape, jnp.float32) * std_dev).astype(jnp.bfloat16)

    return {
        "x_rows": normal(key_x, (TOKENS, D_MODEL), 1.0),
        "adapter_id": draw_adapter_ids(key_ids),
        "w_gate": normal(keys[0], (D_MODEL, D_FF), D_MODEL ** -0.5),
        "w_up": normal(keys[1], (D_MODEL, D_FF), D_MODEL ** -0.5),
        "w_down": normal(keys[2], (D_FF, D_MODEL), D_FF ** -0.5),
        "a_gate": normal(keys[3], (ADAPTERS, D_MODEL, RANK), D_MODEL ** -0.5),
        "b_gate": normal(keys[4], (ADAPTERS, RANK, D_FF), up_std),
        "a_up": normal(keys[5], (ADAPTERS, D_MODEL, RANK), D_MODEL ** -0.5),
        "b_up": normal(keys[6], (ADAPTERS, RANK, D_FF), up_std),
        "a_down": normal(keys[7], (ADAPTERS, D_FF, RANK), D_FF ** -0.5),
        "b_down": normal(keys[8], (ADAPTERS, RANK, D_MODEL), down_std),
    }


def reference(x_rows, adapter_id, w_gate, w_up, w_down, a_gate, b_gate, a_up, b_up, a_down, b_down):
    scale = LORA_ALPHA / RANK
    n_blocks = TOKENS // ROW_BLOCK

    def low_rank(rows_in, block_ids, a_mat, b_mat):
        a_sel = jnp.take(a_mat, block_ids, axis=0).astype(jnp.float32)
        low_proj = jnp.einsum("tk,tkr->tr", rows_in.astype(jnp.float32), a_sel).astype(jnp.bfloat16)
        b_sel = jnp.take(b_mat, block_ids, axis=0).astype(jnp.float32)
        wide_proj = jnp.einsum("tr,trn->tn", low_proj.astype(jnp.float32), b_sel)
        return (scale * wide_proj).astype(jnp.bfloat16).astype(jnp.float32)

    def one_block(block):
        x_blk, block_ids = block
        gate_pre = jnp.dot(x_blk, w_gate, preferred_element_type=jnp.float32) + low_rank(x_blk, block_ids, a_gate, b_gate)
        up_proj = jnp.dot(x_blk, w_up, preferred_element_type=jnp.float32) + low_rank(x_blk, block_ids, a_up, b_up)
        hidden = (jax.nn.silu(gate_pre) * up_proj).astype(jnp.bfloat16)
        down_proj = jnp.dot(hidden, w_down, preferred_element_type=jnp.float32) + low_rank(hidden, block_ids, a_down, b_down)
        return (x_blk.astype(jnp.float32) + down_proj).astype(jnp.bfloat16)

    result = lax.map(one_block, (x_rows.reshape(n_blocks, ROW_BLOCK, D_MODEL), adapter_id.reshape(n_blocks, ROW_BLOCK)))
    return result.reshape(TOKENS, D_MODEL)
```

```python
import functools

import jax
import jax.numpy as jnp
from jax import lax
from jax.experimental import pallas as pl
from jax.experimental.pallas import tpu as pltpu
from jax.sharding import PartitionSpec as P

LORA_ALPHA = 32
PHASES = 2
LANES = 128
TILE = 128
PASS_TILES = 8
BLOCK = 256
F_BLOCK = 1280


def owner_mlp(first_ref, pool_hbm, wg_hbm, wu_hbm, wd_hbm, ag_hbm, bg_hbm, au_hbm, bu_hbm, ad_hbm, bd_hbm, out_hbm,
              starts, pool, slots, x_own, low_g, low_u, acc, acc_low, ag, au, bd, wg, wu, wd, bg, bu, ad, stage,
              pool_sem, fixed_sem, stream_sem, stage_sem, *, scale):
    n_local, d_model, rank = ag.shape
    n_blocks = pool.shape[0] // BLOCK
    n_steps = wg_hbm.shape[1] // F_BLOCK
    cap = PASS_TILES * TILE
    first = first_ref[0].astype(jnp.float32)

    def tile_rows(t):
        return pl.ds(pl.multiple_of(t * TILE, TILE), TILE)

    def block_rows(b):
        return pl.ds(pl.multiple_of(b * BLOCK, BLOCK), BLOCK)

    def load_block(b):
        return pltpu.make_async_copy(pool_hbm.at[block_rows(b), :], pool.at[block_rows(b), :], pool_sem.at[b])

    fixed = [pltpu.make_async_copy(src, dst, fixed_sem.at[i])
             for i, (src, dst) in enumerate(((ag_hbm, ag), (au_hbm, au), (bd_hbm, bd)))]

    def stream(f, s):
        cols = pl.ds(pl.multiple_of(f * F_BLOCK, F_BLOCK), F_BLOCK)
        pairs = ((wg_hbm.at[:, cols], wg), (wu_hbm.at[:, cols], wu), (bg_hbm.at[:, cols], bg),
                 (bu_hbm.at[:, cols], bu), (wd_hbm.at[cols, :], wd), (ad_hbm.at[:, cols, :], ad))
        return [pltpu.make_async_copy(src, dst.at[s], stream_sem.at[s, i]) for i, (src, dst) in enumerate(pairs)]

    def delta(wide):
        return (scale * wide).astype(jnp.bfloat16).astype(jnp.float32)

    for b in range(n_blocks):
        load_block(b).start()
    for copy in fixed:
        copy.start()
    for copy in stream(0, 0):
        copy.start()

    starts[0] = 0
    row = lax.broadcasted_iota(jnp.int32, (BLOCK, BLOCK), 0)
    col = lax.broadcasted_iota(jnp.int32, (BLOCK, BLOCK), 1)
    below = jnp.where(row >= col, 1.0, 0.0).astype(jnp.bfloat16)

    def number(b, c):
        load_block(b).wait()
        local = pool[block_rows(b), d_model:].astype(jnp.float32) - first
        mine = (local >= 0.0) & (local < n_local)
        ones = jnp.where(mine, 1.0, 0.0)
        upto = jnp.dot(below, ones.astype(jnp.bfloat16), preferred_element_type=jnp.float32)
        before = starts[b]
        slots[block_rows(b), :] = jnp.where(mine, upto + (before - 1).astype(jnp.float32), -1.0)
        starts[b + 1] = before + jnp.max(upto).astype(jnp.int32)
        return c

    lax.fori_loop(0, n_blocks, number, 0)
    owned = starts[n_blocks]
    passes = jnp.maximum(pl.cdiv(owned, cap), 1)

    def one_pass(p, carry):
        base = p * cap
        tiles = jnp.minimum(pl.cdiv(jnp.maximum(owned - base, 0), TILE), PASS_TILES)

        def pick(t, b):
            lane = lax.broadcasted_iota(jnp.int32, (BLOCK, LANES), 1) + (base + t * TILE)
            slot = slots[block_rows(b), :]
            hits = [jnp.where(slot == (lane + k).astype(jnp.float32), 1.0, 0.0) for k in range(0, TILE, LANES)]
            return jnp.concatenate(hits, axis=1).astype(jnp.bfloat16)

        @pl.when(p > 0)
        def _():
            for copy in stream(0, 0):
                copy.start()

        def clear(t, c):
            x_own[tile_rows(t), :] = jnp.zeros((TILE, x_own.shape[1]), x_own.dtype)
            acc[tile_rows(t), :] = jnp.zeros((TILE, acc.shape[1]), jnp.float32)
            acc_low[tile_rows(t), :] = jnp.zeros((TILE, acc_low.shape[1]), jnp.float32)
            return c

        lax.fori_loop(0, tiles, clear, 0)

        def gather(b, c):
            def to_tile(t, d):
                at = base + t * TILE

                @pl.when((starts[b] < at + TILE) & (starts[b + 1] > at))
                def _():
                    rows = lax.dot_general(pick(t, b), pool[block_rows(b), :], (((0,), (0,)), ((), ())),
                                           preferred_element_type=jnp.float32)
                    x_own[tile_rows(t), :] += rows.astype(x_own.dtype)
                return d

            return lax.fori_loop(0, tiles, to_tile, c)

        lax.fori_loop(0, n_blocks, gather, 0)

        @pl.when(p == 0)
        def _():
            for copy in fixed:
                copy.wait()

        def keep(t, a, wide):
            which = x_own[tile_rows(t), d_model:].astype(jnp.float32) - first
            return jnp.where(which == a, wide, 0.0)

        def project(t, c):
            rows = tile_rows(t)
            for a_mat, low in ((ag, low_g), (au, low_u)):
                for a in range(n_local):
                    proj = jnp.dot(x_own[rows, :d_model], a_mat[a], preferred_element_type=jnp.float32)
                    low[rows, a * rank:(a + 1) * rank] = keep(t, a, proj).astype(low.dtype)
            return c

        lax.fori_loop(0, tiles, project, 0)

        def hidden_block(f, c):
            s = lax.rem(f, 2)

            @pl.when(f + 1 < n_steps)
            def _():
                for copy in stream(f + 1, 1 - s):
                    copy.start()

            for copy in stream(f, s):
                copy.wait()

            def mlp(t, d):
                rows = tile_rows(t)
                x = x_own[rows, :d_model]
                gate = jnp.dot(x, wg[s], preferred_element_type=jnp.float32)
                gate += delta(jnp.dot(low_g[rows, :], bg[s], preferred_element_type=jnp.float32))
                up = jnp.dot(x, wu[s], preferred_element_type=jnp.float32)
                up += delta(jnp.dot(low_u[rows, :], bu[s], preferred_element_type=jnp.float32))
                hidden = (jax.nn.silu(gate) * up).astype(jnp.bfloat16)
                acc[rows, :] += jnp.dot(hidden, wd[s], preferred_element_type=jnp.float32)
                a_cat = jnp.concatenate([ad[s, a] for a in range(n_local)], axis=1)
                acc_low[rows, :] += jnp.dot(hidden, a_cat, preferred_element_type=jnp.float32)
                return d

            return lax.fori_loop(0, tiles, mlp, c)

        lax.fori_loop(0, n_steps, hidden_block, 0)

        def finish(t, c):
            rows = tile_rows(t)
            for a in range(n_local):
                cols = slice(a * rank, (a + 1) * rank)
                low_g[rows, cols] = keep(t, a, acc_low[rows, cols]).astype(low_g.dtype)
            y = acc[rows, :] + delta(jnp.dot(low_g[rows, :], bd[...], preferred_element_type=jnp.float32))
            x_own[rows, :d_model] = (x_own[rows, :d_model].astype(jnp.float32) + y).astype(x_own.dtype)
            return c

        lax.fori_loop(0, tiles, finish, 0)

        def flush(b, s):
            return pltpu.make_async_copy(stage.at[s], out_hbm.at[block_rows(b), :], stage_sem.at[s])

        def scatter(b, sent):
            lo, hi = starts[b], starts[b + 1]
            mine = ((hi > base) | (p == 0)) & ((lo < base + cap) | (p == passes - 1))

            @pl.when(mine)
            def _():
                s = lax.rem(sent, 2)

                @pl.when(sent >= 2)
                def _():
                    flush(b, s).wait()

                @pl.when((p > 0) & (lo < base))
                def _():
                    back = pltpu.make_async_copy(out_hbm.at[block_rows(b), :], stage.at[s], stage_sem.at[s])
                    back.start()
                    back.wait()

                @pl.when((p == 0) | (lo >= base))
                def _():
                    stage[s] = jnp.zeros(stage.shape[1:], stage.dtype)

                def from_tile(t, d):
                    at = base + t * TILE

                    @pl.when((lo < at + TILE) & (hi > at))
                    def _():
                        moved = jnp.dot(pick(t, b), x_own[tile_rows(t), :d_model], preferred_element_type=jnp.float32)
                        stage[s] += moved.astype(stage.dtype)
                    return d

                lax.fori_loop(0, tiles, from_tile, 0)
                flush(b, s).start()
            return sent + mine.astype(jnp.int32)

        sent = lax.fori_loop(0, n_blocks, scatter, jnp.int32(0))

        @pl.when(sent >= 1)
        def _():
            flush(0, lax.rem(sent + 1, 2)).wait()

        @pl.when(sent >= 2)
        def _():
            flush(0, lax.rem(sent, 2)).wait()

        return carry

    lax.fori_loop(0, passes, one_pass, 0)


def run_owner(pool, first, w_gate, w_up, w_down, a_gate, b_gate, a_up, b_up, a_down, b_down):
    n_pool, width = pool.shape
    n_local, d_model, rank = a_gate.shape
    d_ff = w_gate.shape[1]
    n_blocks = n_pool // BLOCK
    wide = n_local * rank
    cap = PASS_TILES * TILE
    hbm = pl.BlockSpec(memory_space=pl.ANY)
    flops = 2 * 384 * (3 * d_model * d_ff + 3 * wide * d_ff + 3 * wide * d_model)
    bf16, f32 = jnp.bfloat16, jnp.float32
    return pl.pallas_call(
        functools.partial(owner_mlp, scale=LORA_ALPHA / rank),
        out_shape=jax.ShapeDtypeStruct((n_pool, d_model), pool.dtype),
        in_specs=[pl.BlockSpec(memory_space=pltpu.SMEM)] + [hbm] * 10,
        out_specs=hbm,
        scratch_shapes=[
            pltpu.SMEM((n_blocks + 1,), jnp.int32),
            pltpu.VMEM((n_pool, width), bf16),
            pltpu.VMEM((n_pool, LANES), f32),
            pltpu.VMEM((cap, width), bf16),
            pltpu.VMEM((cap, wide), bf16),
            pltpu.VMEM((cap, wide), bf16),
            pltpu.VMEM((cap, d_model), f32),
            pltpu.VMEM((cap, wide), f32),
            pltpu.VMEM(a_gate.shape, bf16),
            pltpu.VMEM(a_up.shape, bf16),
            pltpu.VMEM((wide, d_model), bf16),
            pltpu.VMEM((2, d_model, F_BLOCK), bf16),
            pltpu.VMEM((2, d_model, F_BLOCK), bf16),
            pltpu.VMEM((2, F_BLOCK, d_model), bf16),
            pltpu.VMEM((2, wide, F_BLOCK), bf16),
            pltpu.VMEM((2, wide, F_BLOCK), bf16),
            pltpu.VMEM((2, n_local, F_BLOCK, rank), bf16),
            pltpu.VMEM((2, BLOCK, d_model), bf16),
            pltpu.SemaphoreType.DMA((n_blocks,)),
            pltpu.SemaphoreType.DMA((3,)),
            pltpu.SemaphoreType.DMA((2, 6)),
            pltpu.SemaphoreType.DMA((2,)),
        ],
        compiler_params=pltpu.CompilerParams(vmem_limit_bytes=67043328),
        cost_estimate=pl.CostEstimate(flops=flops, bytes_accessed=140_000_000, transcendentals=0),
    )(first, pool, w_gate, w_up, w_down, a_gate, b_gate.reshape(wide, d_ff), a_up, b_up.reshape(wide, d_ff),
      a_down, b_down.reshape(wide, d_model))


def spread_order(adapter_id, parts):
    n_rows = adapter_id.shape[0]
    index = jnp.arange(n_rows)
    ahead = (adapter_id[None, :] < adapter_id[:, None]) | (
        (adapter_id[None, :] == adapter_id[:, None]) & (index[None, :] < index[:, None]))
    rank = jnp.sum(ahead.astype(jnp.int32), axis=1)
    return (rank % parts) * (n_rows // parts) + rank // parts


def solution(mesh):
    n_dp = mesh.shape["dp"]
    tok_axes = ("rep", "dp", "ad")
    row_spec = P(tok_axes, None)
    owned = P("ad", None, None)

    def local_step(x_rows, adapter_id, *weights):
        n_rows, d_model = x_rows.shape
        n_local = weights[3].shape[0]
        part = n_rows // (PHASES * n_dp)
        dest = spread_order(adapter_id, PHASES * n_dp)
        move = (dest[None, :] == jnp.arange(n_rows)[:, None]).astype(jnp.bfloat16)
        tagged = jnp.concatenate(
            [x_rows, jnp.broadcast_to(adapter_id.astype(x_rows.dtype)[:, None], (n_rows, LANES))], axis=1)
        tagged = jnp.dot(move, tagged, preferred_element_type=jnp.float32).astype(x_rows.dtype)
        tagged = tagged.reshape(PHASES, n_dp, part, d_model + LANES)
        first = (lax.axis_index("ad") * n_local).astype(jnp.int32).reshape(1)
        back = []
        spread = [lax.all_to_all(tagged[ph], "dp", 0, 0) for ph in range(PHASES)]
        pools = [lax.all_gather(s.reshape(n_dp * part, -1), "ad", axis=0, tiled=True) for s in spread]
        done = [run_owner(pool, first, *weights) for pool in pools]
        for d in done:
            mine = lax.psum_scatter(d, "ad", scatter_dimension=0, tiled=True)
            back.append(lax.all_to_all(mine.reshape(n_dp, part, d_model), "dp", 0, 0))
        back = jnp.stack(back).reshape(n_rows, d_model)
        return jnp.dot(move.T, back, preferred_element_type=jnp.float32).astype(x_rows.dtype)

    return jax.shard_map(local_step, mesh=mesh,
                         in_specs=(row_spec, P(tok_axes), P(), P(), P(), owned, owned, owned, owned, owned, owned),
                         out_specs=row_spec, check_vma=False)
```

```python
import functools

import jax
import jax.numpy as jnp
from jax import lax
from jax.experimental import pallas as pl
from jax.experimental.pallas import tpu as pltpu
from jax.sharding import PartitionSpec as P

LORA_ALPHA = 32
PHASES = 2
LANES = 128
TILE = 192
MIN_TILES = 2
MAX_TILES = 4
PACK = 256
BLOCK = 256
F_BLOCK = 1280


def owner_mlp(first_ref, pool_hbm, wg_hbm, wu_hbm, wd_hbm, ag_hbm, bg_hbm, au_hbm, bu_hbm, ad_hbm, bd_hbm, out_hbm,
              pool, relative, slots, pick, x_own, low, acc, acc_low, a_in, bd, wg, wu, wd, bg, bu, ad, stage, hidden,
              pool_sem, fixed_sem, stream_sem, stage_sem, *, scale, n_local, rank):
    n_groups, depth, d_model = bd.shape
    per_group = n_local // n_groups
    n_blocks = pool.shape[0] // BLOCK
    n_steps = wg_hbm.shape[1] // F_BLOCK
    first = first_ref[0].astype(jnp.float32)
    f32, bf16 = jnp.float32, jnp.bfloat16

    def block_rows(b):
        return pl.ds(b * BLOCK, BLOCK)

    def tile_rows(t):
        return pl.ds(pl.multiple_of(t * TILE, TILE), TILE)

    def load_block(b):
        return pltpu.make_async_copy(pool_hbm.at[block_rows(b), :], pool.at[block_rows(b), :], pool_sem.at[b])

    fixed = [pltpu.make_async_copy(bd_hbm, bd, fixed_sem.at[0])]
    for k, src in enumerate((ag_hbm, au_hbm)):
        for a in range(n_local):
            dst = a_in.at[a // per_group, :, pl.ds(k * depth + a % per_group * rank, rank)]
            fixed.append(pltpu.make_async_copy(src.at[a], dst, fixed_sem.at[1 + k * n_local + a]))

    def stream(f, s):
        cols = pl.ds(pl.multiple_of(f * F_BLOCK, F_BLOCK), F_BLOCK)
        pairs = [(wg_hbm.at[:, cols], wg.at[s]), (bg_hbm.at[:, :, cols], bg.at[s]),
                 (wu_hbm.at[:, cols], wu.at[s]), (bu_hbm.at[:, :, cols], bu.at[s]), (wd_hbm.at[cols, :], wd.at[s])]
        pairs += [(ad_hbm.at[a, cols, :], ad.at[s, a // per_group, :, pl.ds(a % per_group * rank, rank)])
                  for a in range(n_local)]
        return [pltpu.make_async_copy(src, dst, stream_sem.at[s, i]) for i, (src, dst) in enumerate(pairs)]

    def delta(product):
        return (scale * product).astype(bf16).astype(f32)

    for b in range(n_blocks):
        load_block(b).start()
    lane = jnp.where(lax.broadcasted_iota(jnp.int32, (8, LANES), 1) == 0, 1.0, 0.0).astype(bf16)
    upper = jnp.where(lax.broadcasted_iota(jnp.int32, (BLOCK, BLOCK), 0)
                      <= lax.broadcasted_iota(jnp.int32, (BLOCK, BLOCK), 1), 1.0, 0.0).astype(bf16)
    group = lax.broadcasted_iota(jnp.int32, (8, BLOCK), 0)
    lowest = (group * per_group).astype(f32)
    before = jnp.zeros((8, BLOCK), f32)
    for b in range(n_blocks):
        load_block(b).wait()
    for copy in fixed:
        copy.start()
    for copy in stream(0, 0):
        copy.start()
    for b in range(n_blocks):
        ids = lax.dot_general(lane, pool[block_rows(b), d_model:], (((1,), (1,)), ((), ())), preferred_element_type=f32)
        local = ids - first - lowest
        mine = (local >= 0.0) & (local < per_group) & (group < n_groups)
        upto = jnp.dot(jnp.where(mine, 1.0, 0.0).astype(bf16), upper, preferred_element_type=f32)
        place = jnp.where(mine, upto + (before - 1.0), -1e6)
        for g in range(n_groups):
            relative[g, b:b + 1, :] = place[g:g + 1, :]
        before = before + jnp.broadcast_to(upto[:, BLOCK - 1:], (8, BLOCK))
    begins = [jnp.int32(0)]
    for g in range(n_groups):
        begins.append(begins[-1] + pl.cdiv(jnp.max(before[g:g + 1, :]).astype(jnp.int32), TILE))
    slot = relative[0]
    for g in range(1, n_groups):
        slot = jnp.maximum(slot, relative[g] + (begins[g] * TILE).astype(f32))
    slots[...] = slot
    passes = jnp.maximum(pl.cdiv(begins[-1], MAX_TILES), 1)

    def one_pass(p, carry):
        tiles = jnp.where(begins[-1] - p * MAX_TILES > MIN_TILES, MAX_TILES, MIN_TILES)

        def group_of(t):
            at = t + p * MAX_TILES
            return sum([(at >= begins[g]).astype(jnp.int32) for g in range(1, n_groups)], jnp.int32(0))

        @pl.when(p > 0)
        def _():
            for copy in stream(0, 0):
                copy.start()

        def gather(t, c):
            rows = tile_rows(t)
            target = (lax.broadcasted_iota(jnp.int32, (TILE, BLOCK), 0) + (p * MAX_TILES + t) * TILE).astype(f32)
            for b in range(n_blocks):
                hit = jnp.broadcast_to(slots[b:b + 1, :], (TILE, BLOCK)) == target
                pick[rows, b * BLOCK:(b + 1) * BLOCK] = jnp.where(hit, 1.0, 0.0).astype(bf16)
            x_own[rows, :] = jnp.dot(pick[rows, :], pool[...], preferred_element_type=f32).astype(bf16)
            acc[rows, :] = jnp.zeros((TILE, d_model), f32)
            acc_low[rows, :] = jnp.zeros((TILE, depth), f32)
            return c

        lax.fori_loop(0, tiles, gather, 0)

        @pl.when(p == 0)
        def _():
            for copy in fixed:
                copy.wait()

        def keep(t, product):
            which = x_own[tile_rows(t), d_model:].astype(f32) - first - (group_of(t) * per_group).astype(f32)
            parts = [jnp.where(which == a, product[:, a * rank:(a + 1) * rank], 0.0) for a in range(per_group)]
            return jnp.concatenate(parts, axis=1).astype(bf16)

        def project(t, c):
            rows = tile_rows(t)
            proj = jnp.dot(x_own[rows, :d_model], a_in[group_of(t)], preferred_element_type=f32)
            for k in range(2):
                low[k, rows, :] = keep(t, proj[:, k * depth:(k + 1) * depth])
            return c

        lax.fori_loop(0, tiles, project, 0)

        def hidden_block(f, c):
            s = lax.rem(f, 2)

            @pl.when(f + 1 < n_steps)
            def _():
                for copy in stream(f + 1, 1 - s):
                    copy.start()

            for copy in stream(f, s):
                copy.wait()

            def mlp(u, d):
                tiles_of = [u * MIN_TILES + k for k in range(MIN_TILES)]
                rows = pl.ds(pl.multiple_of(u * (MIN_TILES * TILE), TILE), MIN_TILES * TILE)
                x = x_own[rows, :d_model]

                def deltas(k, b_mat):
                    return jnp.concatenate([delta(jnp.dot(low[k, tile_rows(t), :], b_mat[s, group_of(t)],
                                                          preferred_element_type=f32)) for t in tiles_of], axis=0)

                gate = jnp.dot(x, wg[s], preferred_element_type=f32) + deltas(0, bg)
                up = jnp.dot(x, wu[s], preferred_element_type=f32) + deltas(1, bu)
                hidden[...] = (jax.nn.silu(gate) * up).astype(bf16)
                acc[rows, :] += jnp.dot(hidden[...], wd[s], preferred_element_type=f32)
                for k, t in enumerate(tiles_of):
                    acc_low[tile_rows(t), :] += jnp.dot(hidden[k * TILE:(k + 1) * TILE, :], ad[s, group_of(t)],
                                                        preferred_element_type=f32)
                return d

            return lax.fori_loop(0, lax.div(tiles, MIN_TILES), mlp, c)

        lax.fori_loop(0, n_steps, hidden_block, 0)

        def finish(t, c):
            rows = tile_rows(t)
            y = acc[rows, :] + delta(jnp.dot(keep(t, acc_low[rows, :]), bd[group_of(t)], preferred_element_type=f32))
            x_own[rows, :d_model] = (x_own[rows, :d_model].astype(f32) + y).astype(bf16)
            return c

        lax.fori_loop(0, tiles, finish, 0)

        def moved(n_rows, cols):
            return lax.dot_general(pick[:n_rows, cols], x_own[:n_rows, :d_model], (((0,), (0,)), ((), ())),
                                   preferred_element_type=f32).astype(bf16)

        small = (p == 0) & (tiles == MIN_TILES)

        @pl.when(small)
        def _():
            def flush(b):
                return pltpu.make_async_copy(stage.at[b % 2], out_hbm.at[block_rows(b), :], stage_sem.at[b % 2])

            for b in range(n_blocks):
                if b >= 2:
                    flush(b - 2).wait()
                stage[b % 2] = moved(MIN_TILES * TILE, block_rows(b))
                flush(b).start()
            flush(n_blocks - 2).wait()
            flush(n_blocks - 1).wait()

        @pl.when(jnp.logical_not(small))
        def _():
            def blank(t, c):
                pick[tile_rows(t), :] = jnp.zeros((TILE, pick.shape[1]), bf16)
                x_own[tile_rows(t), :] = jnp.zeros((TILE, x_own.shape[1]), bf16)
                return c

            lax.fori_loop(tiles, MAX_TILES, blank, 0)

            def block(b, c):
                at = pl.ds(pl.multiple_of(b * BLOCK, BLOCK), BLOCK)
                stage[0] = jnp.zeros(stage.shape[1:], bf16)

                @pl.when(p > 0)
                def _():
                    back = pltpu.make_async_copy(out_hbm.at[at, :], stage.at[0], stage_sem.at[0])
                    back.start()
                    back.wait()

                stage[0] = stage[0] + moved(MAX_TILES * TILE, at)
                put = pltpu.make_async_copy(stage.at[0], out_hbm.at[at, :], stage_sem.at[0])
                put.start()
                put.wait()
                return c

            lax.fori_loop(0, n_blocks, block, 0)

        return carry

    lax.fori_loop(0, passes, one_pass, 0)


def run_owner(pool, first, w_gate, w_up, w_down, a_gate, b_gate, a_up, b_up, a_down, b_down):
    n_pool, width = pool.shape
    n_local, d_model, rank = a_gate.shape
    d_ff = w_gate.shape[1]
    n_blocks = n_pool // BLOCK
    per_group = min(n_local, max(1, PACK // rank))
    n_groups, depth = n_local // per_group, per_group * rank
    rows = MAX_TILES * TILE
    hbm = pl.BlockSpec(memory_space=pl.ANY)
    flops = 2 * MIN_TILES * TILE * (3 * d_model * d_ff + 3 * depth * d_ff + 3 * depth * d_model)
    bf16, f32 = jnp.bfloat16, jnp.float32
    return pl.pallas_call(
        functools.partial(owner_mlp, scale=LORA_ALPHA / rank, n_local=n_local, rank=rank),
        out_shape=jax.ShapeDtypeStruct((n_pool, d_model), pool.dtype),
        in_specs=[pl.BlockSpec(memory_space=pltpu.SMEM)] + [hbm] * 10,
        out_specs=hbm,
        scratch_shapes=[
            pltpu.VMEM((n_pool, width), bf16),
            pltpu.VMEM((n_groups, n_blocks, BLOCK), f32),
            pltpu.VMEM((n_blocks, BLOCK), f32),
            pltpu.VMEM((rows, n_pool), bf16),
            pltpu.VMEM((rows, width), bf16),
            pltpu.VMEM((2, rows, depth), bf16),
            pltpu.VMEM((rows, d_model), f32),
            pltpu.VMEM((rows, depth), f32),
            pltpu.VMEM((n_groups, d_model, 2 * depth), bf16),
            pltpu.VMEM((n_groups, depth, d_model), bf16),
            pltpu.VMEM((2, d_model, F_BLOCK), bf16),
            pltpu.VMEM((2, d_model, F_BLOCK), bf16),
            pltpu.VMEM((2, F_BLOCK, d_model), bf16),
            pltpu.VMEM((2, n_groups, depth, F_BLOCK), bf16),
            pltpu.VMEM((2, n_groups, depth, F_BLOCK), bf16),
            pltpu.VMEM((2, n_groups, F_BLOCK, depth), bf16),
            pltpu.VMEM((2, BLOCK, d_model), bf16),
            pltpu.VMEM((MIN_TILES * TILE, F_BLOCK), bf16),
            pltpu.SemaphoreType.DMA((n_blocks,)),
            pltpu.SemaphoreType.DMA((2 * n_local + 1,)),
            pltpu.SemaphoreType.DMA((2, 5 + n_local)),
            pltpu.SemaphoreType.DMA((2,)),
        ],
        compiler_params=pltpu.CompilerParams(vmem_limit_bytes=67043328),
        cost_estimate=pl.CostEstimate(flops=flops, bytes_accessed=140_000_000, transcendentals=0),
    )(first, pool, w_gate, w_up, w_down, a_gate, b_gate.reshape(n_groups, depth, d_ff),
      a_up, b_up.reshape(n_groups, depth, d_ff), a_down, b_down.reshape(n_groups, depth, d_model))


def spread_order(adapter_id, parts):
    n_rows = adapter_id.shape[0]
    index = jnp.arange(n_rows)
    ahead = (adapter_id[None, :] < adapter_id[:, None]) | (
        (adapter_id[None, :] == adapter_id[:, None]) & (index[None, :] < index[:, None]))
    rank = jnp.sum(ahead.astype(jnp.int32), axis=1)
    return (rank % parts) * (n_rows // parts) + rank // parts


def solution(mesh):
    n_dp = mesh.shape["dp"]
    tok_axes = ("rep", "dp", "ad")
    row_spec = P(tok_axes, None)
    owned = P("ad", None, None)

    def local_step(x_rows, adapter_id, *weights):
        n_rows, d_model = x_rows.shape
        n_local = weights[3].shape[0]
        part = n_rows // (PHASES * n_dp)
        dest = spread_order(adapter_id, PHASES * n_dp)
        move = (dest[None, :] == jnp.arange(n_rows)[:, None]).astype(jnp.bfloat16)
        tagged = jnp.concatenate(
            [x_rows, jnp.broadcast_to(adapter_id.astype(x_rows.dtype)[:, None], (n_rows, LANES))], axis=1)
        tagged = jnp.dot(move, tagged, preferred_element_type=jnp.float32).astype(x_rows.dtype)
        tagged = tagged.reshape(PHASES, n_dp, part, d_model + LANES)
        first = (lax.axis_index("ad") * n_local).astype(jnp.int32).reshape(1)
        back = []
        spread = [lax.all_to_all(tagged[ph], "dp", 0, 0) for ph in range(PHASES)]
        pools = [lax.all_gather(s.reshape(n_dp * part, -1), "ad", axis=0, tiled=True) for s in spread]
        done = [run_owner(pool, first, *weights) for pool in pools]
        for d in done:
            mine = lax.psum_scatter(d, "ad", scatter_dimension=0, tiled=True)
            back.append(lax.all_to_all(mine.reshape(n_dp, part, d_model), "dp", 0, 0))
        back = jnp.stack(back).reshape(n_rows, d_model)
        return jnp.dot(move.T, back, preferred_element_type=jnp.float32).astype(x_rows.dtype)

    return jax.shard_map(local_step, mesh=mesh,
                         in_specs=(row_spec, P(tok_axes), P(), P(), P(), owned, owned, owned, owned, owned, owned),
                         out_specs=row_spec, check_vma=False)
```

```python
import functools

import jax
import jax.numpy as jnp
from jax import lax
from jax.experimental import pallas as pl
from jax.experimental.pallas import tpu as pltpu
from jax.sharding import PartitionSpec as P

LORA_ALPHA = 32
PHASES = 2
LANES = 128
TILE = 192
MIN_TILES = 2
MAX_TILES = 4
PACK = 256
BLOCK = 256
F_BLOCK = 1280


def owner_mlp(first_ref, pool_hbm, wg_hbm, wu_hbm, wd_hbm, ag_hbm, bg_hbm, au_hbm, bu_hbm, ad_hbm, bd_hbm, out_hbm,
              pool, relative, slots, pick, x_own, low, acc, acc_low, a_in, bd, wg, wu, wd, bg, bu, ad, stage, hidden,
              pool_sem, fixed_sem, stream_sem, stage_sem, *, scale, n_local, rank):
    n_groups, depth, d_model = bd.shape
    per_group = n_local // n_groups
    n_blocks = pool.shape[0] // BLOCK
    n_steps = wg_hbm.shape[1] // F_BLOCK
    first = first_ref[0].astype(jnp.float32)
    f32, bf16 = jnp.float32, jnp.bfloat16

    def block_rows(b):
        return pl.ds(b * BLOCK, BLOCK)

    def tile_rows(t):
        return pl.ds(pl.multiple_of(t * TILE, TILE), TILE)

    def load_block(b):
        return pltpu.make_async_copy(pool_hbm.at[block_rows(b), :], pool.at[block_rows(b), :], pool_sem.at[b])

    fixed = [pltpu.make_async_copy(bd_hbm, bd, fixed_sem.at[0])]
    for k, src in enumerate((ag_hbm, au_hbm)):
        for a in range(n_local):
            dst = a_in.at[a // per_group, :, pl.ds(k * depth + a % per_group * rank, rank)]
            fixed.append(pltpu.make_async_copy(src.at[a], dst, fixed_sem.at[1 + k * n_local + a]))

    def stream(f, s):
        cols = pl.ds(pl.multiple_of(f * F_BLOCK, F_BLOCK), F_BLOCK)
        pairs = [(wg_hbm.at[:, cols], wg.at[s]), (bg_hbm.at[:, :, cols], bg.at[s]),
                 (wu_hbm.at[:, cols], wu.at[s]), (bu_hbm.at[:, :, cols], bu.at[s]), (wd_hbm.at[cols, :], wd.at[s])]
        pairs += [(ad_hbm.at[a, cols, :], ad.at[s, a // per_group, :, pl.ds(a % per_group * rank, rank)])
                  for a in range(n_local)]
        return [pltpu.make_async_copy(src, dst, stream_sem.at[s, i]) for i, (src, dst) in enumerate(pairs)]

    def delta(product):
        return (scale * product).astype(bf16).astype(f32)

    for b in range(n_blocks):
        load_block(b).start()
    lane = jnp.where(lax.broadcasted_iota(jnp.int32, (8, LANES), 1) == 0, 1.0, 0.0).astype(bf16)
    upper = jnp.where(lax.broadcasted_iota(jnp.int32, (BLOCK, BLOCK), 0)
                      <= lax.broadcasted_iota(jnp.int32, (BLOCK, BLOCK), 1), 1.0, 0.0).astype(bf16)
    group = lax.broadcasted_iota(jnp.int32, (8, BLOCK), 0)
    lowest = (group * per_group).astype(f32)
    before = jnp.zeros((8, BLOCK), f32)
    for b in range(n_blocks):
        load_block(b).wait()
    for copy in fixed:
        copy.start()
    for copy in stream(0, 0):
        copy.start()
    for b in range(n_blocks):
        ids = lax.dot_general(lane, pool[block_rows(b), d_model:], (((1,), (1,)), ((), ())), preferred_element_type=f32)
        local = ids - first - lowest
        mine = (local >= 0.0) & (local < per_group) & (group < n_groups)
        upto = jnp.dot(jnp.where(mine, 1.0, 0.0).astype(bf16), upper, preferred_element_type=f32)
        place = jnp.where(mine, upto + (before - 1.0), -1e6)
        for g in range(n_groups):
            relative[g, b:b + 1, :] = place[g:g + 1, :]
        before = before + jnp.broadcast_to(upto[:, BLOCK - 1:], (8, BLOCK))
    begins = [jnp.int32(0)]
    for g in range(n_groups):
        begins.append(begins[-1] + pl.cdiv(jnp.max(before[g:g + 1, :]).astype(jnp.int32), TILE))
    slot = relative[0]
    for g in range(1, n_groups):
        slot = jnp.maximum(slot, relative[g] + (begins[g] * TILE).astype(f32))
    slots[...] = slot
    passes = jnp.maximum(pl.cdiv(begins[-1], MAX_TILES), 1)

    def one_pass(p, carry):
        tiles = jnp.where(begins[-1] - p * MAX_TILES > MIN_TILES, MAX_TILES, MIN_TILES)

        def group_of(t):
            at = t + p * MAX_TILES
            return sum([(at >= begins[g]).astype(jnp.int32) for g in range(1, n_groups)], jnp.int32(0))

        @pl.when(p > 0)
        def _():
            for copy in stream(0, 0):
                copy.start()

        def gather(t, c):
            rows = tile_rows(t)
            target = (lax.broadcasted_iota(jnp.int32, (TILE, BLOCK), 0) + (p * MAX_TILES + t) * TILE).astype(f32)
            for b in range(n_blocks):
                hit = jnp.broadcast_to(slots[b:b + 1, :], (TILE, BLOCK)) == target
                pick[rows, b * BLOCK:(b + 1) * BLOCK] = jnp.where(hit, 1.0, 0.0).astype(bf16)
            x_own[rows, :] = jnp.dot(pick[rows, :], pool[...], preferred_element_type=f32).astype(bf16)
            acc[rows, :] = jnp.zeros((TILE, d_model), f32)
            acc_low[rows, :] = jnp.zeros((TILE, depth), f32)
            return c

        lax.fori_loop(0, tiles, gather, 0)

        @pl.when(p == 0)
        def _():
            for copy in fixed:
                copy.wait()

        def keep(t, product):
            which = x_own[tile_rows(t), d_model:].astype(f32) - first - (group_of(t) * per_group).astype(f32)
            parts = [jnp.where(which == a, product[:, a * rank:(a + 1) * rank], 0.0) for a in range(per_group)]
            return jnp.concatenate(parts, axis=1).astype(bf16)

        def project(t, c):
            rows = tile_rows(t)
            proj = jnp.dot(x_own[rows, :d_model], a_in[group_of(t)], preferred_element_type=f32)
            for k in range(2):
                low[k, rows, :] = keep(t, proj[:, k * depth:(k + 1) * depth])
            return c

        lax.fori_loop(0, tiles, project, 0)

        def hidden_block(f, c):
            s = lax.rem(f, 2)

            @pl.when(f + 1 < n_steps)
            def _():
                for copy in stream(f + 1, 1 - s):
                    copy.start()

            for copy in stream(f, s):
                copy.wait()

            def mlp(u, d):
                tiles_of = [u * MIN_TILES + k for k in range(MIN_TILES)]
                rows = pl.ds(pl.multiple_of(u * (MIN_TILES * TILE), TILE), MIN_TILES * TILE)
                x = x_own[rows, :d_model]

                def deltas(k, b_mat):
                    return jnp.concatenate([delta(jnp.dot(low[k, tile_rows(t), :], b_mat[s, group_of(t)],
                                                          preferred_element_type=f32)) for t in tiles_of], axis=0)

                gate = jnp.dot(x, wg[s], preferred_element_type=f32) + deltas(0, bg)
                up = jnp.dot(x, wu[s], preferred_element_type=f32) + deltas(1, bu)
                hidden[...] = (jax.nn.silu(gate) * up).astype(bf16)
                acc[rows, :] += jnp.dot(hidden[...], wd[s], preferred_element_type=f32)
                for k, t in enumerate(tiles_of):
                    acc_low[tile_rows(t), :] += jnp.dot(hidden[k * TILE:(k + 1) * TILE, :], ad[s, group_of(t)],
                                                        preferred_element_type=f32)
                return d

            return lax.fori_loop(0, lax.div(tiles, MIN_TILES), mlp, c)

        lax.fori_loop(0, n_steps, hidden_block, 0)

        def finish(t, c):
            rows = tile_rows(t)
            y = acc[rows, :] + delta(jnp.dot(keep(t, acc_low[rows, :]), bd[group_of(t)], preferred_element_type=f32))
            x_own[rows, :d_model] = (x_own[rows, :d_model].astype(f32) + y).astype(bf16)
            return c

        lax.fori_loop(0, tiles, finish, 0)

        def moved(n_rows, cols):
            return lax.dot_general(pick[:n_rows, cols], x_own[:n_rows, :d_model], (((0,), (0,)), ((), ())),
                                   preferred_element_type=f32).astype(bf16)

        small = (p == 0) & (tiles == MIN_TILES)

        @pl.when(small)
        def _():
            def flush(b):
                return pltpu.make_async_copy(stage.at[b % 2], out_hbm.at[block_rows(b), :], stage_sem.at[b % 2])

            for b in range(n_blocks):
                if b >= 2:
                    flush(b - 2).wait()
                stage[b % 2] = moved(MIN_TILES * TILE, block_rows(b))
                flush(b).start()
            flush(n_blocks - 2).wait()
            flush(n_blocks - 1).wait()

        @pl.when(jnp.logical_not(small))
        def _():
            def blank(t, c):
                pick[tile_rows(t), :] = jnp.zeros((TILE, pick.shape[1]), bf16)
                x_own[tile_rows(t), :] = jnp.zeros((TILE, x_own.shape[1]), bf16)
                return c

            lax.fori_loop(tiles, MAX_TILES, blank, 0)

            def block(b, c):
                at = pl.ds(pl.multiple_of(b * BLOCK, BLOCK), BLOCK)
                stage[0] = jnp.zeros(stage.shape[1:], bf16)

                @pl.when(p > 0)
                def _():
                    back = pltpu.make_async_copy(out_hbm.at[at, :], stage.at[0], stage_sem.at[0])
                    back.start()
                    back.wait()

                stage[0] = stage[0] + moved(MAX_TILES * TILE, at)
                put = pltpu.make_async_copy(stage.at[0], out_hbm.at[at, :], stage_sem.at[0])
                put.start()
                put.wait()
                return c

            lax.fori_loop(0, n_blocks, block, 0)

        return carry

    lax.fori_loop(0, passes, one_pass, 0)


def run_owner(pool, first, w_gate, w_up, w_down, a_gate, b_gate, a_up, b_up, a_down, b_down):
    n_pool, width = pool.shape
    n_local, d_model, rank = a_gate.shape
    d_ff = w_gate.shape[1]
    n_blocks = n_pool // BLOCK
    per_group = min(n_local, max(1, PACK // rank))
    n_groups, depth = n_local // per_group, per_group * rank
    rows = MAX_TILES * TILE
    hbm = pl.BlockSpec(memory_space=pl.ANY)
    flops = 2 * MIN_TILES * TILE * (3 * d_model * d_ff + 3 * depth * d_ff + 3 * depth * d_model)
    bf16, f32 = jnp.bfloat16, jnp.float32
    return pl.pallas_call(
        functools.partial(owner_mlp, scale=LORA_ALPHA / rank, n_local=n_local, rank=rank),
        out_shape=jax.ShapeDtypeStruct((n_pool, d_model), pool.dtype),
        in_specs=[pl.BlockSpec(memory_space=pltpu.SMEM)] + [hbm] * 10,
        out_specs=hbm,
        scratch_shapes=[
            pltpu.VMEM((n_pool, width), bf16),
            pltpu.VMEM((n_groups, n_blocks, BLOCK), f32),
            pltpu.VMEM((n_blocks, BLOCK), f32),
            pltpu.VMEM((rows, n_pool), bf16),
            pltpu.VMEM((rows, width), bf16),
            pltpu.VMEM((2, rows, depth), bf16),
            pltpu.VMEM((rows, d_model), f32),
            pltpu.VMEM((rows, depth), f32),
            pltpu.VMEM((n_groups, d_model, 2 * depth), bf16),
            pltpu.VMEM((n_groups, depth, d_model), bf16),
            pltpu.VMEM((2, d_model, F_BLOCK), bf16),
            pltpu.VMEM((2, d_model, F_BLOCK), bf16),
            pltpu.VMEM((2, F_BLOCK, d_model), bf16),
            pltpu.VMEM((2, n_groups, depth, F_BLOCK), bf16),
            pltpu.VMEM((2, n_groups, depth, F_BLOCK), bf16),
            pltpu.VMEM((2, n_groups, F_BLOCK, depth), bf16),
            pltpu.VMEM((2, BLOCK, d_model), bf16),
            pltpu.VMEM((MIN_TILES * TILE, F_BLOCK), bf16),
            pltpu.SemaphoreType.DMA((n_blocks,)),
            pltpu.SemaphoreType.DMA((2 * n_local + 1,)),
            pltpu.SemaphoreType.DMA((2, 5 + n_local)),
            pltpu.SemaphoreType.DMA((2,)),
        ],
        compiler_params=pltpu.CompilerParams(vmem_limit_bytes=67043328),
        cost_estimate=pl.CostEstimate(flops=flops, bytes_accessed=140_000_000, transcendentals=0),
    )(first, pool, w_gate, w_up, w_down, a_gate, b_gate.reshape(n_groups, depth, d_ff),
      a_up, b_up.reshape(n_groups, depth, d_ff), a_down, b_down.reshape(n_groups, depth, d_model))


def spread_kernel(rows_ref, pool_ref, later_ref, send_sem, recv_sem, own_sem):
    n_ad, n_dp, part, _ = pool_ref.shape
    n_later = later_ref.shape[0]
    half = part // 2
    dp, ad = lax.axis_index("dp"), lax.axis_index("ad")
    core = lax.rem(ad, 2)
    other = ad + 1 - 2 * core
    right = lax.rem(ad + 2, n_ad)
    left = lax.rem(ad + n_ad - 2, n_ad)
    far = lax.rem(ad + 4, n_ad)

    barrier = pltpu.get_barrier_semaphore()
    peers = [{"dp": lax.rem(dp + r, n_dp)} for r in range(1, n_dp)] + [{"ad": right}, {"ad": left}, {"ad": other}]
    for peer in peers:
        pl.semaphore_signal(barrier, inc=1, device_id=peer, device_id_type=pl.DeviceIdType.MESH)
    pl.semaphore_wait(barrier, len(peers))

    def remote(kind, r, src, dst, peer):
        return pltpu.make_async_remote_copy(
            src_ref=src, dst_ref=dst, send_sem=send_sem.at[kind, r], recv_sem=recv_sem.at[kind, r],
            device_id=peer, device_id_type=pl.DeviceIdType.MESH)

    def source(r):
        return lax.rem(dp + n_dp - r, n_dp)

    def across(phase, r):
        to = lax.rem(dp + r, n_dp)
        dst = pool_ref.at[ad, dp] if phase == 0 else later_ref.at[phase - 1, dp]
        return remote(9 + phase, r, rows_ref.at[phase, to], dst, {"dp": to})

    def whole(kind, r, block, peer):
        src = rows_ref.at[0, dp] if r == 0 and kind in (0, 1, 2) else pool_ref.at[block, source(r)]
        return remote(kind, r, src, pool_ref.at[block, source(r)], peer)

    def halved(kind, r, block, which, peer):
        at = pool_ref.at[block, source(r), pl.ds(which * half, half), :]
        return remote(kind, r, at, at, peer)

    def near(r):
        return [whole(0, r, ad, {"ad": right}), whole(1, r, ad, {"ad": left}), whole(2, r, ad, {"ad": other})]

    def on_right(r):
        return [halved(3, r, left, 0, {"ad": right}), whole(4, r, left, {"ad": other})]

    def on_left(r):
        return [halved(5, r, right, 1, {"ad": left}), whole(6, r, right, {"ad": other})]

    def on_far(r, which):
        return [halved(7 + which, r, far, which, {"ad": other})]

    def start(copies):
        for copy in copies:
            copy.start()

    own = [pltpu.make_async_copy(rows_ref.at[0, dp], pool_ref.at[ad, dp], own_sem.at[0])]
    own += [pltpu.make_async_copy(rows_ref.at[p + 1, dp], later_ref.at[p, dp], own_sem.at[p + 1]) for p in range(n_later)]
    order = [0] + sorted(range(1, n_dp), key=lambda r: min(r, n_dp - r))
    start(near(0))
    for r in order[1:]:
        across(0, r).start()
    start(own)
    for phase in range(1, n_later + 1):
        for r in order[1:]:
            across(phase, r).start()

    def hand_on(r):
        near(r)[0].wait_recv()
        start(on_right(r))
        near(r)[1].wait_recv()
        start(on_left(r))

    def hand_over(r):
        on_right(r)[0].wait_recv()
        start(on_far(r, 0))
        on_left(r)[0].wait_recv()
        start(on_far(r, 1))

    for n in range(n_dp + 2):
        if 0 < n < n_dp:
            across(0, order[n]).wait_recv()
            start(near(order[n]))
        if 0 <= n - 1 < n_dp:
            hand_on(order[n - 1])
        if 0 <= n - 2 < n_dp:
            hand_over(order[n - 2])
    for copy in own:
        copy.wait()
    for r in order:
        copies = near(r) + on_right(r) + on_left(r) + on_far(r, 0) + on_far(r, 1)
        for copy in copies:
            copy.wait_send()
        for copy in (near(r)[2], on_right(r)[1], on_left(r)[1], on_far(r, 0)[0], on_far(r, 1)[0]):
            copy.wait_recv()
        if r:
            across(0, r).wait_send()
            for phase in range(1, n_later + 1):
                across(phase, r).wait()


def run_spread(tagged, n_ad):
    phases, n_dp, part, width = tagged.shape
    kinds = 9 + phases
    hbm = pl.BlockSpec(memory_space=pl.ANY)
    return pl.pallas_call(
        spread_kernel,
        out_shape=(jax.ShapeDtypeStruct((n_ad, n_dp, part, width), tagged.dtype),
                   jax.ShapeDtypeStruct((phases - 1, n_dp, part, width), tagged.dtype)),
        in_specs=[pl.BlockSpec(memory_space=pltpu.VMEM)],
        out_specs=(hbm, hbm),
        scratch_shapes=[
            pltpu.SemaphoreType.DMA((kinds, n_dp)),
            pltpu.SemaphoreType.DMA((kinds, n_dp)),
            pltpu.SemaphoreType.DMA((phases,)),
        ],
        compiler_params=pltpu.CompilerParams(collective_id=0, has_side_effects=True),
    )(tagged)


def spread_order(adapter_id, parts):
    n_rows = adapter_id.shape[0]
    index = jnp.arange(n_rows)
    ahead = (adapter_id[None, :] < adapter_id[:, None]) | (
        (adapter_id[None, :] == adapter_id[:, None]) & (index[None, :] < index[:, None]))
    rank = jnp.sum(ahead.astype(jnp.int32), axis=1)
    return (rank % parts) * (n_rows // parts) + rank // parts


def solution(mesh):
    n_dp, n_ad = mesh.shape["dp"], mesh.shape["ad"]
    tok_axes = ("rep", "dp", "ad")
    row_spec = P(tok_axes, None)
    owned = P("ad", None, None)

    def local_step(x_rows, adapter_id, *weights):
        n_rows, d_model = x_rows.shape
        n_local = weights[3].shape[0]
        part = n_rows // (PHASES * n_dp)
        dest = spread_order(adapter_id, PHASES * n_dp)
        move = (dest[None, :] == jnp.arange(n_rows)[:, None]).astype(jnp.bfloat16)
        tagged = jnp.concatenate(
            [x_rows, jnp.broadcast_to(adapter_id.astype(x_rows.dtype)[:, None], (n_rows, LANES))], axis=1)
        tagged = jnp.dot(move, tagged, preferred_element_type=jnp.float32).astype(x_rows.dtype)
        tagged = tagged.reshape(PHASES, n_dp, part, d_model + LANES)
        first = (lax.axis_index("ad") * n_local).astype(jnp.int32).reshape(1)
        back = []
        pool, later = run_spread(tagged, n_ad)
        pools = [pool.reshape(n_ad * n_dp * part, -1)]
        pools += [lax.all_gather(later[p].reshape(n_dp * part, -1), "ad", axis=0, tiled=True) for p in range(PHASES - 1)]
        done = [run_owner(pool, first, *weights) for pool in pools]
        for d in done:
            mine = lax.psum_scatter(d, "ad", scatter_dimension=0, tiled=True)
            back.append(lax.all_to_all(mine.reshape(n_dp, part, d_model), "dp", 0, 0))
        back = jnp.stack(back).reshape(n_rows, d_model)
        return jnp.dot(move.T, back, preferred_element_type=jnp.float32).astype(x_rows.dtype)

    return jax.shard_map(local_step, mesh=mesh,
                         in_specs=(row_spec, P(tok_axes), P(), P(), P(), owned, owned, owned, owned, owned, owned),
                         out_specs=row_spec, check_vma=False)
```

```python
import functools

import jax
import jax.numpy as jnp
from jax import lax
from jax.experimental import pallas as pl
from jax.experimental.pallas import tpu as pltpu
from jax.sharding import PartitionSpec as P

LORA_ALPHA = 32
PHASES = 2
LANES = 128
TILE = 192
MIN_TILES = 2
MAX_TILES = 4
PACK = 256
BLOCK = 256
F_BLOCK = 1280


def owner_mlp(first_ref, pool_hbm, wg_hbm, wu_hbm, wd_hbm, ag_hbm, bg_hbm, au_hbm, bu_hbm, ad_hbm, bd_hbm, out_hbm,
              pool, relative, slots, pick, x_own, low, acc, acc_low, a_in, bd, wg, wu, wd, bg, bu, ad, stage, hidden,
              pool_sem, fixed_sem, stream_sem, stage_sem, *, scale, n_local, rank):
    n_groups, depth, d_model = bd.shape
    per_group = n_local // n_groups
    n_blocks = pool.shape[0] // BLOCK
    n_steps = wg_hbm.shape[1] // F_BLOCK
    first = first_ref[0].astype(jnp.float32)
    f32, bf16 = jnp.float32, jnp.bfloat16

    def block_rows(b):
        return pl.ds(b * BLOCK, BLOCK)

    def tile_rows(t):
        return pl.ds(pl.multiple_of(t * TILE, TILE), TILE)

    def load_block(b):
        return pltpu.make_async_copy(pool_hbm.at[block_rows(b), :], pool.at[block_rows(b), :], pool_sem.at[b])

    fixed = [pltpu.make_async_copy(bd_hbm, bd, fixed_sem.at[0])]
    for k, src in enumerate((ag_hbm, au_hbm)):
        for a in range(n_local):
            dst = a_in.at[a // per_group, :, pl.ds(k * depth + a % per_group * rank, rank)]
            fixed.append(pltpu.make_async_copy(src.at[a], dst, fixed_sem.at[1 + k * n_local + a]))

    def stream(f, s):
        cols = pl.ds(pl.multiple_of(f * F_BLOCK, F_BLOCK), F_BLOCK)
        pairs = [(wg_hbm.at[:, cols], wg.at[s]), (bg_hbm.at[:, :, cols], bg.at[s]),
                 (wu_hbm.at[:, cols], wu.at[s]), (bu_hbm.at[:, :, cols], bu.at[s]), (wd_hbm.at[cols, :], wd.at[s])]
        pairs += [(ad_hbm.at[a, cols, :], ad.at[s, a // per_group, :, pl.ds(a % per_group * rank, rank)])
                  for a in range(n_local)]
        return [pltpu.make_async_copy(src, dst, stream_sem.at[s, i]) for i, (src, dst) in enumerate(pairs)]

    def delta(product):
        return (scale * product).astype(bf16).astype(f32)

    for b in range(n_blocks):
        load_block(b).start()
    lane = jnp.where(lax.broadcasted_iota(jnp.int32, (8, LANES), 1) == 0, 1.0, 0.0).astype(bf16)
    upper = jnp.where(lax.broadcasted_iota(jnp.int32, (BLOCK, BLOCK), 0)
                      <= lax.broadcasted_iota(jnp.int32, (BLOCK, BLOCK), 1), 1.0, 0.0).astype(bf16)
    group = lax.broadcasted_iota(jnp.int32, (8, BLOCK), 0)
    lowest = (group * per_group).astype(f32)
    before = jnp.zeros((8, BLOCK), f32)
    for b in range(n_blocks):
        load_block(b).wait()
        if b == n_blocks // 2:
            for copy in fixed + stream(0, 0):
                copy.start()
    ids = lax.dot_general(lane, pool[:, d_model:], (((1,), (1,)), ((), ())), preferred_element_type=f32)
    mine = []
    for b in range(n_blocks):
        local = ids[:, b * BLOCK:(b + 1) * BLOCK] - first - lowest
        mine.append((local >= 0.0) & (local < per_group) & (group < n_groups))
    ones = jnp.concatenate([jnp.where(m, 1.0, 0.0) for m in mine], axis=0).astype(bf16)
    counts = jnp.dot(ones, upper, preferred_element_type=f32)
    for b in range(n_blocks):
        upto = counts[8 * b:8 * (b + 1), :]
        place = jnp.where(mine[b], upto + (before - 1.0), -1e6)
        for g in range(n_groups):
            relative[g, b:b + 1, :] = place[g:g + 1, :]
        before = before + jnp.broadcast_to(upto[:, BLOCK - 1:], (8, BLOCK))
    begins = [jnp.int32(0)]
    for g in range(n_groups):
        begins.append(begins[-1] + pl.cdiv(jnp.max(before[g:g + 1, :]).astype(jnp.int32), TILE))
    slot = relative[0]
    for g in range(1, n_groups):
        slot = jnp.maximum(slot, relative[g] + (begins[g] * TILE).astype(f32))
    slots[...] = slot
    passes = jnp.maximum(pl.cdiv(begins[-1], MAX_TILES), 1)

    def one_pass(p, carry):
        tiles = jnp.where(begins[-1] - p * MAX_TILES > MIN_TILES, MAX_TILES, MIN_TILES)

        def group_of(t):
            at = t + p * MAX_TILES
            return sum([(at >= begins[g]).astype(jnp.int32) for g in range(1, n_groups)], jnp.int32(0))

        @pl.when(p > 0)
        def _():
            for copy in stream(0, 0):
                copy.start()

        def gather(t, c):
            rows = tile_rows(t)
            target = (lax.broadcasted_iota(jnp.int32, (TILE, BLOCK), 0) + (p * MAX_TILES + t) * TILE).astype(f32)
            for b in range(n_blocks):
                hit = jnp.broadcast_to(slots[b:b + 1, :], (TILE, BLOCK)) == target
                pick[rows, b * BLOCK:(b + 1) * BLOCK] = jnp.where(hit, 1.0, 0.0).astype(bf16)
            x_own[rows, :] = jnp.dot(pick[rows, :], pool[...], preferred_element_type=f32).astype(bf16)
            acc[rows, :] = jnp.zeros((TILE, d_model), f32)
            acc_low[rows, :] = jnp.zeros((TILE, depth), f32)
            return c

        lax.fori_loop(0, tiles, gather, 0)

        @pl.when(p == 0)
        def _():
            for copy in fixed:
                copy.wait()

        def keep(t, product):
            which = x_own[tile_rows(t), d_model:].astype(f32) - first - (group_of(t) * per_group).astype(f32)
            parts = [jnp.where(which == a, product[:, a * rank:(a + 1) * rank], 0.0) for a in range(per_group)]
            return jnp.concatenate(parts, axis=1).astype(bf16)

        def project(t, c):
            rows = tile_rows(t)
            proj = jnp.dot(x_own[rows, :d_model], a_in[group_of(t)], preferred_element_type=f32)
            for k in range(2):
                low[k, rows, :] = keep(t, proj[:, k * depth:(k + 1) * depth])
            return c

        lax.fori_loop(0, tiles, project, 0)

        def hidden_block(f, c):
            s = lax.rem(f, 2)

            @pl.when(f + 1 < n_steps)
            def _():
                for copy in stream(f + 1, 1 - s):
                    copy.start()

            for copy in stream(f, s):
                copy.wait()

            def mlp(u, d):
                tiles_of = [u * MIN_TILES + k for k in range(MIN_TILES)]
                rows = pl.ds(pl.multiple_of(u * (MIN_TILES * TILE), TILE), MIN_TILES * TILE)
                x = x_own[rows, :d_model]

                def deltas(k, b_mat):
                    return jnp.concatenate([delta(jnp.dot(low[k, tile_rows(t), :], b_mat[s, group_of(t)],
                                                          preferred_element_type=f32)) for t in tiles_of], axis=0)

                gate = jnp.dot(x, wg[s], preferred_element_type=f32) + deltas(0, bg)
                up = jnp.dot(x, wu[s], preferred_element_type=f32) + deltas(1, bu)
                hidden[...] = (jax.nn.silu(gate) * up).astype(bf16)
                acc[rows, :] += jnp.dot(hidden[...], wd[s], preferred_element_type=f32)
                for k, t in enumerate(tiles_of):
                    acc_low[tile_rows(t), :] += jnp.dot(hidden[k * TILE:(k + 1) * TILE, :], ad[s, group_of(t)],
                                                        preferred_element_type=f32)
                return d

            return lax.fori_loop(0, lax.div(tiles, MIN_TILES), mlp, c)

        lax.fori_loop(0, n_steps, hidden_block, 0)

        def finish(t, c):
            rows = tile_rows(t)
            y = acc[rows, :] + delta(jnp.dot(keep(t, acc_low[rows, :]), bd[group_of(t)], preferred_element_type=f32))
            x_own[rows, :d_model] = (x_own[rows, :d_model].astype(f32) + y).astype(bf16)
            return c

        lax.fori_loop(0, tiles, finish, 0)

        def moved(n_rows, cols):
            return lax.dot_general(pick[:n_rows, cols], x_own[:n_rows, :d_model], (((0,), (0,)), ((), ())),
                                   preferred_element_type=f32).astype(bf16)

        small = (p == 0) & (tiles == MIN_TILES)

        @pl.when(small)
        def _():
            def flush(b):
                return pltpu.make_async_copy(stage.at[b % 2], out_hbm.at[block_rows(b), :], stage_sem.at[b % 2])

            for b in range(n_blocks):
                if b >= 2:
                    flush(b - 2).wait()
                stage[b % 2] = moved(MIN_TILES * TILE, block_rows(b))
                flush(b).start()
            flush(n_blocks - 2).wait()
            flush(n_blocks - 1).wait()

        @pl.when(jnp.logical_not(small))
        def _():
            def blank(t, c):
                pick[tile_rows(t), :] = jnp.zeros((TILE, pick.shape[1]), bf16)
                x_own[tile_rows(t), :] = jnp.zeros((TILE, x_own.shape[1]), bf16)
                return c

            lax.fori_loop(tiles, MAX_TILES, blank, 0)

            def block(b, c):
                at = pl.ds(pl.multiple_of(b * BLOCK, BLOCK), BLOCK)
                stage[0] = jnp.zeros(stage.shape[1:], bf16)

                @pl.when(p > 0)
                def _():
                    back = pltpu.make_async_copy(out_hbm.at[at, :], stage.at[0], stage_sem.at[0])
                    back.start()
                    back.wait()

                stage[0] = stage[0] + moved(MAX_TILES * TILE, at)
                put = pltpu.make_async_copy(stage.at[0], out_hbm.at[at, :], stage_sem.at[0])
                put.start()
                put.wait()
                return c

            lax.fori_loop(0, n_blocks, block, 0)

        return carry

    lax.fori_loop(0, passes, one_pass, 0)


def run_owner(pool, first, w_gate, w_up, w_down, a_gate, b_gate, a_up, b_up, a_down, b_down):
    n_pool, width = pool.shape
    n_local, d_model, rank = a_gate.shape
    d_ff = w_gate.shape[1]
    n_blocks = n_pool // BLOCK
    per_group = min(n_local, max(1, PACK // rank))
    n_groups, depth = n_local // per_group, per_group * rank
    rows = MAX_TILES * TILE
    hbm = pl.BlockSpec(memory_space=pl.ANY)
    flops = 2 * MIN_TILES * TILE * (3 * d_model * d_ff + 3 * depth * d_ff + 3 * depth * d_model)
    bf16, f32 = jnp.bfloat16, jnp.float32
    return pl.pallas_call(
        functools.partial(owner_mlp, scale=LORA_ALPHA / rank, n_local=n_local, rank=rank),
        out_shape=jax.ShapeDtypeStruct((n_pool, d_model), pool.dtype),
        in_specs=[pl.BlockSpec(memory_space=pltpu.SMEM)] + [hbm] * 10,
        out_specs=hbm,
        scratch_shapes=[
            pltpu.VMEM((n_pool, width), bf16),
            pltpu.VMEM((n_groups, n_blocks, BLOCK), f32),
            pltpu.VMEM((n_blocks, BLOCK), f32),
            pltpu.VMEM((rows, n_pool), bf16),
            pltpu.VMEM((rows, width), bf16),
            pltpu.VMEM((2, rows, depth), bf16),
            pltpu.VMEM((rows, d_model), f32),
            pltpu.VMEM((rows, depth), f32),
            pltpu.VMEM((n_groups, d_model, 2 * depth), bf16),
            pltpu.VMEM((n_groups, depth, d_model), bf16),
            pltpu.VMEM((2, d_model, F_BLOCK), bf16),
            pltpu.VMEM((2, d_model, F_BLOCK), bf16),
            pltpu.VMEM((2, F_BLOCK, d_model), bf16),
            pltpu.VMEM((2, n_groups, depth, F_BLOCK), bf16),
            pltpu.VMEM((2, n_groups, depth, F_BLOCK), bf16),
            pltpu.VMEM((2, n_groups, F_BLOCK, depth), bf16),
            pltpu.VMEM((2, BLOCK, d_model), bf16),
            pltpu.VMEM((MIN_TILES * TILE, F_BLOCK), bf16),
            pltpu.SemaphoreType.DMA((n_blocks,)),
            pltpu.SemaphoreType.DMA((2 * n_local + 1,)),
            pltpu.SemaphoreType.DMA((2, 5 + n_local)),
            pltpu.SemaphoreType.DMA((2,)),
        ],
        compiler_params=pltpu.CompilerParams(vmem_limit_bytes=67043328),
        cost_estimate=pl.CostEstimate(flops=flops, bytes_accessed=140_000_000, transcendentals=0),
    )(first, pool, w_gate, w_up, w_down, a_gate, b_gate.reshape(n_groups, depth, d_ff),
      a_up, b_up.reshape(n_groups, depth, d_ff), a_down, b_down.reshape(n_groups, depth, d_model))


def spread_kernel(rows_ref, pool_ref, later_ref, send_sem, recv_sem, own_sem):
    n_ad, n_dp, part, _ = pool_ref.shape
    n_later = later_ref.shape[0]
    half = part // 2
    dp, ad = lax.axis_index("dp"), lax.axis_index("ad")
    core = lax.rem(ad, 2)
    other = ad + 1 - 2 * core
    right = lax.rem(ad + 2, n_ad)
    left = lax.rem(ad + n_ad - 2, n_ad)
    far = lax.rem(ad + 4, n_ad)

    barrier = pltpu.get_barrier_semaphore()
    peers = [{"dp": lax.rem(dp + r, n_dp)} for r in range(1, n_dp)] + [{"ad": right}, {"ad": left}, {"ad": other}]
    for peer in peers:
        pl.semaphore_signal(barrier, inc=1, device_id=peer, device_id_type=pl.DeviceIdType.MESH)
    pl.semaphore_wait(barrier, len(peers))

    def remote(kind, r, src, dst, peer):
        return pltpu.make_async_remote_copy(
            src_ref=src, dst_ref=dst, send_sem=send_sem.at[kind, r], recv_sem=recv_sem.at[kind, r],
            device_id=peer, device_id_type=pl.DeviceIdType.MESH)

    def source(r):
        return lax.rem(dp + n_dp - r, n_dp)

    def across(phase, r):
        to = lax.rem(dp + r, n_dp)
        dst = pool_ref.at[ad, dp] if phase == 0 else later_ref.at[phase - 1, dp]
        return remote(9 + phase, r, rows_ref.at[phase, to], dst, {"dp": to})

    def whole(kind, r, block, peer):
        src = rows_ref.at[0, dp] if r == 0 and kind in (0, 1, 2) else pool_ref.at[block, source(r)]
        return remote(kind, r, src, pool_ref.at[block, source(r)], peer)

    def halved(kind, r, block, which, peer):
        at = pool_ref.at[block, source(r), pl.ds(which * half, half), :]
        return remote(kind, r, at, at, peer)

    def near(r):
        return [whole(0, r, ad, {"ad": right}), whole(1, r, ad, {"ad": left}), whole(2, r, ad, {"ad": other})]

    def on_right(r):
        return [halved(3, r, left, 0, {"ad": right}), whole(4, r, left, {"ad": other})]

    def on_left(r):
        return [halved(5, r, right, 1, {"ad": left}), whole(6, r, right, {"ad": other})]

    def on_far(r, which):
        return [halved(7 + which, r, far, which, {"ad": other})]

    def start(copies):
        for copy in copies:
            copy.start()

    own = [pltpu.make_async_copy(rows_ref.at[0, dp], pool_ref.at[ad, dp], own_sem.at[0])]
    own += [pltpu.make_async_copy(rows_ref.at[p + 1, dp], later_ref.at[p, dp], own_sem.at[p + 1]) for p in range(n_later)]
    order = [0] + sorted(range(1, n_dp), key=lambda r: min(r, n_dp - r))
    start(near(0))
    for r in order[1:]:
        across(0, r).start()
    start(own)
    for phase in range(1, n_later + 1):
        for r in order[1:]:
            across(phase, r).start()

    def hand_on(r):
        near(r)[0].wait_recv()
        start(on_right(r))
        near(r)[1].wait_recv()
        start(on_left(r))

    def hand_over(r):
        on_right(r)[0].wait_recv()
        start(on_far(r, 0))
        on_left(r)[0].wait_recv()
        start(on_far(r, 1))

    for n in range(n_dp + 2):
        if 0 < n < n_dp:
            across(0, order[n]).wait_recv()
            start(near(order[n]))
        if 0 <= n - 1 < n_dp:
            hand_on(order[n - 1])
        if 0 <= n - 2 < n_dp:
            hand_over(order[n - 2])
    for copy in own:
        copy.wait()
    for r in order:
        copies = near(r) + on_right(r) + on_left(r) + on_far(r, 0) + on_far(r, 1)
        for copy in copies:
            copy.wait_send()
        for copy in (near(r)[2], on_right(r)[1], on_left(r)[1], on_far(r, 0)[0], on_far(r, 1)[0]):
            copy.wait_recv()
        if r:
            across(0, r).wait_send()
            for phase in range(1, n_later + 1):
                across(phase, r).wait()


def run_spread(tagged, n_ad):
    phases, n_dp, part, width = tagged.shape
    kinds = 9 + phases
    hbm = pl.BlockSpec(memory_space=pl.ANY)
    return pl.pallas_call(
        spread_kernel,
        out_shape=(jax.ShapeDtypeStruct((n_ad, n_dp, part, width), tagged.dtype),
                   jax.ShapeDtypeStruct((phases - 1, n_dp, part, width), tagged.dtype)),
        in_specs=[pl.BlockSpec(memory_space=pltpu.VMEM)],
        out_specs=(hbm, hbm),
        scratch_shapes=[
            pltpu.SemaphoreType.DMA((kinds, n_dp)),
            pltpu.SemaphoreType.DMA((kinds, n_dp)),
            pltpu.SemaphoreType.DMA((phases,)),
        ],
        compiler_params=pltpu.CompilerParams(collective_id=0, has_side_effects=True),
    )(tagged)


def return_kernel(rows_ref, out_ref, send_sem, recv_sem, own_sem):
    n_dp = rows_ref.shape[0]
    dp = lax.axis_index("dp")
    barrier = pltpu.get_barrier_semaphore()
    for r in range(1, n_dp):
        pl.semaphore_signal(barrier, inc=1, device_id={"dp": lax.rem(dp + r, n_dp)},
                            device_id_type=pl.DeviceIdType.MESH)
    pl.semaphore_wait(barrier, n_dp - 1)
    copies = [pltpu.make_async_copy(rows_ref.at[dp], out_ref.at[dp], own_sem)]
    for r in sorted(range(1, n_dp), key=lambda r: -min(r, n_dp - r)):
        to = lax.rem(dp + r, n_dp)
        copies.append(pltpu.make_async_remote_copy(
            src_ref=rows_ref.at[to], dst_ref=out_ref.at[dp], send_sem=send_sem.at[r], recv_sem=recv_sem.at[r],
            device_id={"dp": to}, device_id_type=pl.DeviceIdType.MESH))
    for copy in copies[1:] + copies[:1]:
        copy.start()
    for copy in copies:
        copy.wait()


def run_return(rows):
    n_dp = rows.shape[0]
    return pl.pallas_call(
        return_kernel,
        out_shape=jax.ShapeDtypeStruct(rows.shape, rows.dtype),
        in_specs=[pl.BlockSpec(memory_space=pltpu.VMEM)],
        out_specs=pl.BlockSpec(memory_space=pl.ANY),
        scratch_shapes=[pltpu.SemaphoreType.DMA((n_dp,)), pltpu.SemaphoreType.DMA((n_dp,)), pltpu.SemaphoreType.DMA],
        compiler_params=pltpu.CompilerParams(collective_id=1, has_side_effects=True),
    )(rows)


def spread_order(adapter_id, parts):
    n_rows = adapter_id.shape[0]
    index = jnp.arange(n_rows)
    ahead = (adapter_id[None, :] < adapter_id[:, None]) | (
        (adapter_id[None, :] == adapter_id[:, None]) & (index[None, :] < index[:, None]))
    rank = jnp.sum(ahead.astype(jnp.int32), axis=1)
    return (rank % parts) * (n_rows // parts) + rank // parts


def solution(mesh):
    n_dp, n_ad = mesh.shape["dp"], mesh.shape["ad"]
    tok_axes = ("rep", "dp", "ad")
    row_spec = P(tok_axes, None)
    owned = P("ad", None, None)

    def local_step(x_rows, adapter_id, *weights):
        n_rows, d_model = x_rows.shape
        n_local = weights[3].shape[0]
        part = n_rows // (PHASES * n_dp)
        dest = spread_order(adapter_id, PHASES * n_dp)
        move = (dest[None, :] == jnp.arange(n_rows)[:, None]).astype(jnp.bfloat16)
        tagged = jnp.concatenate(
            [x_rows, jnp.broadcast_to(adapter_id.astype(x_rows.dtype)[:, None], (n_rows, LANES))], axis=1)
        tagged = jnp.dot(move, tagged, preferred_element_type=jnp.float32).astype(x_rows.dtype)
        tagged = tagged.reshape(PHASES, n_dp, part, d_model + LANES)
        first = (lax.axis_index("ad") * n_local).astype(jnp.int32).reshape(1)
        back = []
        pool, later = run_spread(tagged, n_ad)
        pools = [pool.reshape(n_ad * n_dp * part, -1)]
        pools += [lax.all_gather(later[p].reshape(n_dp * part, -1), "ad", axis=0, tiled=True) for p in range(PHASES - 1)]
        done = [run_owner(pool, first, *weights) for pool in pools]
        for ph, d in enumerate(done):
            mine = lax.psum_scatter(d, "ad", scatter_dimension=0, tiled=True).reshape(n_dp, part, d_model)
            back.append(run_return(mine) if ph == PHASES - 1 else lax.all_to_all(mine, "dp", 0, 0))
        back = jnp.stack(back).reshape(n_rows, d_model)
        return jnp.dot(move.T, back, preferred_element_type=jnp.float32).astype(x_rows.dtype)

    return jax.shard_map(local_step, mesh=mesh,
                         in_specs=(row_spec, P(tok_axes), P(), P(), P(), owned, owned, owned, owned, owned, owned),
                         out_specs=row_spec, check_vma=False)
```
